32 devices in a mesh: rep: 2 (over z, core), dp: 16 (over x, y).
Axes of the slice: x: 4, y: 4, z: 1, core: 2. Of those that a mesh axis runs over, the one named last changes fastest.
The devices are a block of a 4x4x8 slice.
Arguments:
- a: bfloat16 [32, 4, 4096, 640], P(('rep', 'dp')), parts along dimension 0
- g: bfloat16 [32, 4, 4096, 2048], P(('rep', 'dp')), parts along dimension 0
Outputs:
- output: bfloat16 [8, 640, 2048], P('rep'), parts along dimension 0
There are 2 independent parts. The reference program is written for one: setup_inputs(seed, part) draws one part's arguments, and reference() takes and returns one part's arrays. A program takes and returns all parts, laid end to end along the dimension named above; each array names one.
All inputs are finite; a program needn't handle non-finite values.
Results may differ from the reference program's by a relative error of at most 0.012.
Values are sent between devices in bfloat16 or wider.
A program may use at most 768 MiB of HBM per device.

```python
import jax
import jax.numpy as jnp
from jax import lax

DEVICES = 16
MATRICES = 4
TOKENS = 4096
D = 640
FF = 2048


def setup_inputs(seed: int = 0, part: int = 0) -> dict:
    ka, kg, ks = (jax.random.fold_in(k, part) for k in jax.random.split(jax.random.key(seed), 3))
    size = 2.0 ** jax.random.uniform(ks, (DEVICES, MATRICES, 1, 1), jnp.float32, -1.0, 1.0)
    a = jax.random.normal(ka, (DEVICES, MATRICES, TOKENS, D), jnp.float32)
    g = size * jax.random.normal(kg, (DEVICES, MATRICES, TOKENS, FF), jnp.float32) * (DEVICES * TOKENS) ** -0.5
    return {"a": a.astype(jnp.bfloat16), "g": g.astype(jnp.bfloat16)}


def reference(a, g):
    def take(so_far, one):
        return so_far + jnp.einsum("ntd,ntf->ndf", *one, preferred_element_type=jnp.float32), None

    return lax.scan(take, jnp.zeros((MATRICES, D, FF), jnp.float32), (a, g))[0].astype(jnp.bfloat16)
```

```python
import functools
import math

import jax
import jax.numpy as jnp
from jax import lax
from jax.experimental import pallas as pl
from jax.experimental.pallas import tpu as pltpu
from jax.sharding import PartitionSpec as P

MESH = pl.DeviceIdType.MESH
F32, BF16 = jnp.float32, jnp.bfloat16
LANES = 128
GBUFS = 3
COMBINE1, OWN1, COMBINE2, OWN2, PASS2, SEND1 = 2, 4, 6, 8, 10, 12
PASS1, DONE1 = 2, 4


def kernel(side, chunks_per, a_ref, g_ref, out_ref, abuf, gbuf, acc, own, send1, recv1, part2, send2, recv2, obuf,
           asem, gsem, osem, ssem, rsem):
    mats, tokens, d = a_ref.shape
    chunks = mats * chunks_per
    half = d // 2
    quarter = half // side
    width = side * LANES
    strip = g_ref.shape[2] // side
    me = lax.axis_index("dp")
    pos = (me // side, lax.rem(me, side))
    core = lax.rem(lax.axis_index("rep"), 2)

    def device(axis, index):
        return {"dp": index * side + pos[1] if axis == 0 else pos[0] * side + index}

    def wrap(i):
        return lax.rem(i, side)

    def block(i, size):
        return pl.ds(pl.multiple_of(i * size, size), size)

    def parity(c):
        return lax.rem(c + core, 2)

    def to(axis, index, src, dst, kind, h, c):
        return pltpu.make_async_remote_copy(
            src_ref=src, dst_ref=dst, send_sem=ssem.at[kind, h, c], recv_sem=rsem.at[kind, h, c],
            device_id=device(axis, index), device_id_type=MESH)

    def copy_a(n):
        i = lax.rem(n, 2)
        return pltpu.make_async_copy(a_ref.at[n], abuf.at[i], asem.at[i])

    def copy_g(t, b):
        n, j, i = t // chunks_per, lax.rem(t, chunks_per), lax.rem(t, GBUFS)
        cols = pl.ds(pl.multiple_of(b * strip + j * LANES, LANES), LANES)
        return pltpu.make_async_copy(g_ref.at[n, :, cols], gbuf.at[i, :, pl.ds(b * LANES, LANES)], gsem.at[i])

    def whole_g(t):
        i = lax.rem(t, GBUFS)
        return pltpu.make_async_copy(g_ref.at[0, :, pl.ds(0, width)], gbuf.at[i], gsem.at[i])

    def start_g(t):
        for b in range(side):
            copy_g(t, b).start()

    def hop1(kind, h, c):
        p, s = pos[h], 1 + 2 * parity(c)
        index = wrap(p + s) if kind == 1 else wrap(p + side - s)
        return to(h, index, send1.at[kind, h, c], recv1.at[kind, h, c], kind, h, c)

    def matmul(t):
        n = t // chunks_per
        acc[...] = lax.dot_general(abuf[lax.rem(n, 2)], gbuf[lax.rem(t, GBUFS)], (((0,), (0,)), ((), ())),
                                   preferred_element_type=F32)
        r = lax.rem(t, OWN1)
        for h in range(2):
            rows = pl.ds(h * half, half)
            p, s = pos[h], 1 + 2 * parity(t)
            send1[0, h, t] = acc[rows, block(wrap(p + 2), LANES)].astype(BF16)
            send1[1, h, t] = acc[rows, block(wrap(p + s), LANES)].astype(BF16)
            own[r, h, 0] = acc[rows, block(wrap(p + side - s), LANES)]
            own[r, h, 1] = acc[rows, block(p, LANES)]

    def start1(t):
        for h in range(2):
            hop1(0, h, t).start()
            hop1(1, h, t).start()

    def combine1(c):
        r = lax.rem(c, OWN1)
        for h in range(2):
            hop1(0, h, c).wait_recv()
            send1[2, h, c] = (own[r, h, 0] + recv1[0, h, c].astype(F32)).astype(BF16)
            hop1(2, h, c).start()

    def hop2(kind, h, c):
        q, s = pos[1 - h], 1 + 2 * parity(c)
        index = wrap(q + s) if kind == 1 else wrap(q + side - s)
        return to(1 - h, index, send2.at[kind, h, c], recv2.at[kind, h, c], 3 + kind, h, c)

    def own1(c):
        r, r2 = lax.rem(c, OWN1), lax.rem(c, OWN2 - OWN1)
        for h in range(2):
            q, s = pos[1 - h], 1 + 2 * parity(c)
            hop1(1, h, c).wait_recv()
            hop1(2, h, c).wait_recv()
            part2[r2, h] = own[r, h, 1] + recv1[1, h, c].astype(F32) + recv1[2, h, c].astype(F32)
            send2[0, h, c] = part2[r2, h, block(wrap(q + 2), quarter)].astype(BF16)
            send2[1, h, c] = part2[r2, h, block(wrap(q + s), quarter)].astype(BF16)
            hop2(0, h, c).start()
            hop2(1, h, c).start()

    def combine2(c):
        r2 = lax.rem(c, OWN2 - OWN1)
        for h in range(2):
            q, s = pos[1 - h], 1 + 2 * parity(c)
            hop2(0, h, c).wait_recv()
            mine = part2[r2, h, block(wrap(q + side - s), quarter)]
            send2[2, h, c] = (mine + recv2[0, h, c].astype(F32)).astype(BF16)
            hop2(2, h, c).start()

    def columns(b, c):
        return pl.ds(pl.multiple_of(b * strip + lax.rem(c, chunks_per) * LANES, LANES), LANES)

    def gather2(kind, h, c):
        q, s = pos[1 - h], 1 + 2 * parity(c)
        owner = wrap(q + side - s) if kind == 2 else q
        index = wrap(q + (1, side - 1, s)[kind])
        rows = pl.ds(pl.multiple_of(h * half + owner * quarter, 16), quarter)
        ref = obuf.at[c // chunks_per, rows, columns(pos[h], c)]
        return to(1 - h, index, ref, ref, 6 + kind, h, c)

    def wait2(kind, h, c):
        ref = obuf.at[c // chunks_per, pl.ds(h * half, quarter), columns(pos[h], c)]
        pltpu.make_async_remote_copy(src_ref=ref, dst_ref=ref, send_sem=ssem.at[6, h, c], recv_sem=rsem.at[6 + kind, h, c],
                                     device_id=device(0, pos[0]), device_id_type=MESH).wait_recv()

    def own2(c):
        r2 = lax.rem(c, OWN2 - OWN1)
        for h in range(2):
            q = pos[1 - h]
            hop2(1, h, c).wait_recv()
            hop2(2, h, c).wait_recv()
            total = part2[r2, h, block(q, quarter)] + recv2[1, h, c].astype(F32) + recv2[2, h, c].astype(F32)
            rows = pl.ds(pl.multiple_of(h * half + q * quarter, 16), quarter)
            obuf[c // chunks_per, rows, columns(pos[h], c)] = total.astype(BF16)
            gather2(0, h, c).start()
            gather2(1, h, c).start()

    def pass2(c):
        for h in range(2):
            wait2(parity(c), h, c)
            gather2(2, h, c).start()

    def gather1(kind, h, c):
        p, s = pos[h], 1 + 2 * parity(c)
        owner = wrap(p + side - s) if kind == 2 else p
        index = wrap(p + (1, side - 1, s)[kind])
        ref = obuf.at[c // chunks_per, pl.ds(h * half, half), columns(owner, c)]
        return to(h, index, ref, ref, 9 + kind, h, c)

    def wait1(kind, h, c):
        ref = obuf.at[c // chunks_per, pl.ds(h * half, half), columns(pos[h], c)]
        pltpu.make_async_remote_copy(src_ref=ref, dst_ref=ref, send_sem=ssem.at[9, h, c], recv_sem=rsem.at[9 + kind, h, c],
                                     device_id=device(0, pos[0]), device_id_type=MESH).wait_recv()

    def send_whole(c):
        for h in range(2):
            wait2(1 - parity(c), h, c)
            wait2(2, h, c)
            gather1(0, h, c).start()
            gather1(1, h, c).start()

    def pass1(c):
        for h in range(2):
            wait1(parity(c), h, c)
            gather1(2, h, c).start()

    def copy_out(b, c):
        ref = (c // chunks_per, slice(None), columns(b, c))
        return pltpu.make_async_copy(obuf.at[ref], out_ref.at[ref], osem.at[b, c])

    def done1(c):
        for h in range(2):
            wait1(1 - parity(c), h, c)
            wait1(2, h, c)
        for b in range(side):
            copy_out(b, c).start()

    def when(step, c, last):
        @pl.when((c >= 0) & (c < last))
        def _():
            step(c)

    def reduce_steps(t):
        for step, lag in ((pass2, PASS2), (own2, OWN2), (combine2, COMBINE2), (own1, OWN1), (combine1, COMBINE1)):
            when(step, t - lag, chunks)

    barrier = pltpu.get_barrier_semaphore()
    neighbours = [device(axis, wrap(pos[axis] + k)) for axis in range(2) for k in (1, side - 1)]
    for nb in neighbours:
        pl.semaphore_signal(barrier, inc=1, device_id=nb, device_id_type=MESH)
    copy_a(0).start()
    for t in range(GBUFS - 1):
        start_g(t)

    start_g(GBUFS - 1)
    copy_a(0).wait()
    copy_a(1).start()
    whole_g(0).wait()
    matmul(0)
    pl.semaphore_wait(barrier, len(neighbours))
    start1(0)

    def compute_slot(t, carry):
        reduce_steps(t)

        @pl.when(t + GBUFS - 1 < chunks)
        def _():
            start_g(t + GBUFS - 1)

        @pl.when(lax.rem(t, chunks_per) == 0)
        def _():
            n = t // chunks_per

            @pl.when(n + 1 < mats)
            def _():
                copy_a(n + 1).start()

            copy_a(n).wait()

        whole_g(t).wait()
        matmul(t)
        start1(t)
        return carry

    lax.fori_loop(1, chunks, compute_slot, 0)

    def gather_slot(u, carry):
        reduce_steps(chunks + u)
        when(send_whole, u, chunks)
        when(pass1, u - PASS1, chunks)
        when(done1, u - DONE1, chunks)
        return carry

    lax.fori_loop(0, chunks + DONE1, gather_slot, 0)

    def finish(c, carry):
        for h in range(2):
            for kind in range(3):
                hop1(kind, h, c).wait_send()
                hop2(kind, h, c).wait_send()
                gather2(kind, h, c).wait_send()
                gather1(kind, h, c).wait_send()
        for b in range(side):
            copy_out(b, c).wait()
        return carry

    lax.fori_loop(0, chunks, finish, 0)


def solution(mesh):
    side = math.isqrt(mesh.shape["dp"])

    def local(a, g):
        _, mats, tokens, d = a.shape
        ff = g.shape[3]
        width = side * LANES
        chunks_per = ff // width
        chunks = mats * chunks_per
        half = d // 2
        quarter = half // side
        dma = pltpu.SemaphoreType.DMA
        return pl.pallas_call(
            functools.partial(kernel, side, chunks_per),
            out_shape=jax.ShapeDtypeStruct((mats, d, ff), BF16),
            in_specs=[pl.BlockSpec(memory_space=pltpu.HBM)] * 2,
            out_specs=pl.BlockSpec(memory_space=pltpu.HBM),
            scratch_shapes=[
                pltpu.VMEM((2, tokens, d), BF16),
                pltpu.VMEM((GBUFS, tokens, width), BF16),
                pltpu.VMEM((d, width), F32),
                pltpu.VMEM((OWN1, 2, 2, half, LANES), F32),
                pltpu.VMEM((3, 2, chunks, half, LANES), BF16),
                pltpu.VMEM((3, 2, chunks, half, LANES), BF16),
                pltpu.VMEM((OWN2 - OWN1, 2, half, LANES), F32),
                pltpu.VMEM((3, 2, chunks, quarter, LANES), BF16),
                pltpu.VMEM((3, 2, chunks, quarter, LANES), BF16),
                pltpu.VMEM((mats, d, ff), BF16),
                dma((2,)),
                dma((GBUFS,)),
                dma((side, chunks)),
                dma((12, 2, chunks)),
                dma((12, 2, chunks)),
            ],
            compiler_params=pltpu.CompilerParams(collective_id=0, has_side_effects=True, vmem_limit_bytes=65_000_000),
            cost_estimate=pl.CostEstimate(flops=2 * mats * tokens * d * ff, bytes_accessed=2 * mats * tokens * (d + ff),
                                          transcendentals=0),
            name="weight_gradients",
        )(a[0], g[0])

    return jax.shard_map(local, mesh=mesh, in_specs=(P(("rep", "dp")), P(("rep", "dp"))), out_specs=P("rep"), check_vma=False)
```

```python
import functools
import math

import jax
import jax.numpy as jnp
from jax import lax
from jax.experimental import pallas as pl
from jax.experimental.pallas import tpu as pltpu
from jax.sharding import PartitionSpec as P

MESH = pl.DeviceIdType.MESH
F32, BF16 = jnp.float32, jnp.bfloat16
LANES = 128
GBUFS = 3
GROUP = 2
HEAD = 4
COMBINE1, OWN1, COMBINE2, OWN2, PASS2 = 3, 6, 8, 10, 12
SEND1, PASS1, DONE1 = 16, 3, 6
OWN_RING = OWN1 + GROUP - 1
PART_RING = -(-(OWN2 - OWN1) // GROUP)


def kernel(side, chunks_per, a_ref, g_ref, out, abuf, gbuf, acc, own, send1, recv1, part2, send2, recv2,
           asem, gsem, hsem, ssem, rsem1, rsem2):
    mats, tokens, d = a_ref.shape
    chunks = mats * chunks_per
    groups = chunks // GROUP
    half = d // 2
    quarter = half // side
    width = side * LANES
    strip = g_ref.shape[2] // side
    me = lax.axis_index("dp")
    pos = (me // side, lax.rem(me, side))
    core = lax.rem(lax.axis_index("rep"), 2)

    def device(axis, index):
        return {"dp": index * side + pos[1] if axis == 0 else pos[0] * side + index}

    def wrap(i):
        return lax.rem(i, side)

    def block(i, size):
        return pl.ds(pl.multiple_of(i * size, size), size)

    def parity(c):
        return lax.rem(c + core, 2)

    def step(c):
        return 1 + 2 * parity(c)

    def to(axis, index, src, dst, send_sem, recv_sem):
        return pltpu.make_async_remote_copy(src_ref=src, dst_ref=dst, send_sem=send_sem, recv_sem=recv_sem,
                                            device_id=device(axis, index), device_id_type=MESH)

    def copy_a(n):
        i = lax.rem(n, 2)
        return pltpu.make_async_copy(a_ref.at[n], abuf.at[i], asem.at[i])

    def start_g(t):
        n, j, i = t // chunks_per, lax.rem(t, chunks_per), lax.rem(t, GBUFS)
        for b in range(side):
            cols = pl.ds(pl.multiple_of(b * strip + j * LANES, LANES), LANES)
            pltpu.make_async_copy(g_ref.at[n, :, cols], gbuf.at[i, :, pl.ds(b * LANES, LANES)], gsem.at[i]).start()

    def whole_g(t):
        i = lax.rem(t, GBUFS)
        return pltpu.make_async_copy(g_ref.at[0, :, pl.ds(0, width)], gbuf.at[i], gsem.at[i])

    def head_rows(k):
        return pl.ds(k * (tokens // HEAD), tokens // HEAD)

    def head_a(k):
        return pltpu.make_async_copy(a_ref.at[0, head_rows(k)], abuf.at[0, head_rows(k)], hsem.at[0, k])

    def start_head(k):
        head_a(k).start()
        for b in range(side):
            pltpu.make_async_copy(g_ref.at[0, head_rows(k), pl.ds(b * strip, LANES)],
                                  gbuf.at[0, head_rows(k), pl.ds(b * LANES, LANES)], hsem.at[1, k]).start()

    def wait_head(k):
        head_a(k).wait()
        pltpu.make_async_copy(g_ref.at[0, head_rows(k), pl.ds(0, width)], gbuf.at[0, head_rows(k)], hsem.at[1, k]).wait()

    def product(a, g):
        return lax.dot_general(a, g, (((0,), (0,)), ((), ())), preferred_element_type=F32)

    def hop1(kind, h, c):
        p, s = pos[h], step(c)
        index = wrap(p + s) if kind == 1 else wrap(p + side - s)
        return to(h, index, send1.at[kind, h, c], recv1.at[kind, h, c], ssem.at[0], rsem1.at[kind, h, c])

    def start1(t):
        r = lax.rem(t, OWN_RING)
        for h in range(2):
            rows = pl.ds(h * half, half)
            p, s = pos[h], step(t)
            send1[0, h, t] = acc[rows, block(wrap(p + 2), LANES)].astype(BF16)
            send1[1, h, t] = acc[rows, block(wrap(p + s), LANES)].astype(BF16)
            own[r, h, 0] = acc[rows, block(wrap(p + side - s), LANES)]
            own[r, h, 1] = acc[rows, block(p, LANES)]
        for h in range(2):
            hop1(0, h, t).start()
            hop1(1, h, t).start()

    def combine1(c):
        r = lax.rem(c, OWN_RING)
        for h in range(2):
            hop1(0, h, c).wait_recv()
            send1[2, h, c] = (own[r, h, 0] + recv1[0, h, c].astype(F32)).astype(BF16)
            hop1(2, h, c).start()

    def hop2(kind, h, k):
        q, s = pos[1 - h], step(k)
        index = wrap(q + s) if kind == 1 else wrap(q + side - s)
        return to(1 - h, index, send2.at[kind, h, k], recv2.at[kind, h, k], ssem.at[1], rsem2.at[kind, h, k])

    def own1(k):
        r2 = lax.rem(k, PART_RING)
        for h in range(2):
            q, s = pos[1 - h], step(k)
            for i in range(GROUP):
                c = k * GROUP + i
                hop1(1, h, c).wait_recv()
                hop1(2, h, c).wait_recv()
                part2[r2, h, i] = (own[lax.rem(c, OWN_RING), h, 1] + recv1[1, h, c].astype(F32)
                                   + recv1[2, h, c].astype(F32))
                send2[0, h, k, i] = part2[r2, h, i, block(wrap(q + 2), quarter)].astype(BF16)
                send2[1, h, k, i] = part2[r2, h, i, block(wrap(q + s), quarter)].astype(BF16)
            hop2(0, h, k).start()
            hop2(1, h, k).start()

    def combine2(k):
        r2 = lax.rem(k, PART_RING)
        for h in range(2):
            q, s = pos[1 - h], step(k)
            hop2(0, h, k).wait_recv()
            mine = part2[r2, h, :, block(wrap(q + side - s), quarter)]
            send2[2, h, k] = (mine + recv2[0, h, k].astype(F32)).astype(BF16)
            hop2(2, h, k).start()

    def columns(b, c, count):
        first = b * strip + lax.rem(c, chunks_per) * LANES
        return pl.ds(pl.multiple_of(first, count * LANES), count * LANES)

    def gather2(kind, h, k):
        q, s, c = pos[1 - h], step(k), k * GROUP
        owner = wrap(q + side - s) if kind == 2 else q
        index = wrap(q + (1, side - 1, s)[kind])
        rows = pl.ds(pl.multiple_of(h * half + owner * quarter, 16), quarter)
        ref = out.at[c // chunks_per, rows, columns(pos[h], c, GROUP)]
        return to(1 - h, index, ref, ref, ssem.at[2], rsem2.at[3 + kind, h, k])

    def wait2(kind, h, k):
        c = k * GROUP
        ref = out.at[c // chunks_per, pl.ds(h * half, quarter), columns(pos[h], c, GROUP)]
        to(h, pos[h], ref, ref, ssem.at[2], rsem2.at[3 + kind, h, k]).wait_recv()

    def own2(k):
        r2 = lax.rem(k, PART_RING)
        for h in range(2):
            q = pos[1 - h]
            hop2(1, h, k).wait_recv()
            hop2(2, h, k).wait_recv()
            rows = pl.ds(pl.multiple_of(h * half + q * quarter, 16), quarter)
            for i in range(GROUP):
                c = k * GROUP + i
                total = (part2[r2, h, i, block(q, quarter)] + recv2[1, h, k, i].astype(F32)
                         + recv2[2, h, k, i].astype(F32))
                out[c // chunks_per, rows, columns(pos[h], c, 1)] = total.astype(BF16)
            gather2(0, h, k).start()
            gather2(1, h, k).start()

    def pass2(k):
        for h in range(2):
            wait2(parity(k), h, k)
            gather2(2, h, k).start()

    def gather1(kind, h, k):
        p, s, c = pos[h], step(k), k * GROUP
        owner = wrap(p + side - s) if kind == 2 else p
        index = wrap(p + (1, side - 1, s)[kind])
        ref = out.at[c // chunks_per, pl.ds(h * half, half), columns(owner, c, GROUP)]
        return to(h, index, ref, ref, ssem.at[3], rsem2.at[6 + kind, h, k])

    def wait1(kind, h, k):
        c = k * GROUP
        ref = out.at[c // chunks_per, pl.ds(h * half, half), columns(pos[h], c, GROUP)]
        to(h, pos[h], ref, ref, ssem.at[3], rsem2.at[6 + kind, h, k]).wait_recv()

    def send_whole(k):
        for h in range(2):
            wait2(1 - parity(k), h, k)
            wait2(2, h, k)
            gather1(0, h, k).start()
            gather1(1, h, k).start()

    def pass1(k):
        for h in range(2):
            wait1(parity(k), h, k)
            gather1(2, h, k).start()

    def done1(k):
        for h in range(2):
            wait1(1 - parity(k), h, k)
            wait1(2, h, k)

    def per_chunk(do, c):
        @pl.when((c >= 0) & (c < chunks))
        def _():
            do(c)

    def per_group(do, c):
        k = c // GROUP

        @pl.when((c >= 0) & (k < groups) & (lax.rem(c, GROUP) == 0))
        def _():
            do(k)

    def steps(t):
        per_group(done1, t - SEND1 - DONE1)
        per_group(pass1, t - SEND1 - PASS1)
        per_group(send_whole, t - SEND1)
        per_group(pass2, t - PASS2 - GROUP + 1)
        per_group(own2, t - OWN2 - GROUP + 1)
        per_group(combine2, t - COMBINE2 - GROUP + 1)
        per_group(own1, t - OWN1 - GROUP + 1)
        per_chunk(combine1, t - COMBINE1)

    barrier = pltpu.get_barrier_semaphore()
    neighbours = [device(axis, wrap(pos[axis] + k)) for axis in range(2) for k in (1, side - 1)]
    for nb in neighbours:
        pl.semaphore_signal(barrier, inc=1, device_id=nb, device_id_type=MESH)
    for k in range(HEAD):
        start_head(k)
    for k in range(HEAD):
        wait_head(k)
        if k == 0:
            start_g(1)
        part = product(abuf[0, head_rows(k)], gbuf[0, head_rows(k)])
        acc[...] = part if k == 0 else acc[...] + part
    pl.semaphore_wait(barrier, len(neighbours))
    start1(0)
    start_g(2)
    copy_a(1).start()

    def compute_slot(t, carry):
        steps(t)

        @pl.when(t + GBUFS - 1 < chunks)
        def _():
            start_g(t + GBUFS - 1)

        @pl.when(lax.rem(t, chunks_per) == 0)
        def _():
            n = t // chunks_per

            @pl.when(n + 1 < mats)
            def _():
                copy_a(n + 1).start()

            copy_a(n).wait()

        whole_g(t).wait()
        acc[...] = product(abuf[lax.rem(t // chunks_per, 2)], gbuf[lax.rem(t, GBUFS)])
        start1(t)
        return carry

    lax.fori_loop(1, chunks, compute_slot, 0)

    def gather_slot(t, carry):
        steps(t)
        return carry

    lax.fori_loop(chunks, SEND1 + chunks - GROUP + DONE1 + 1, gather_slot, 0)

    to(0, pos[0], send1, recv1, ssem.at[0], rsem1.at[0, 0, 0]).wait_send()
    to(0, pos[0], send2, recv2, ssem.at[1], rsem2.at[0, 0, 0]).wait_send()
    to(0, pos[0], send2, recv2, ssem.at[2], rsem2.at[0, 0, 0]).wait_send()
    to(0, pos[0], send1, recv1, ssem.at[3], rsem2.at[0, 0, 0]).wait_send()


def solution(mesh):
    side = math.isqrt(mesh.shape["dp"])

    def local(a, g):
        _, mats, tokens, d = a.shape
        ff = g.shape[3]
        width = side * LANES
        chunks_per = ff // width
        chunks = mats * chunks_per
        groups = chunks // GROUP
        half = d // 2
        quarter = half // side
        dma = pltpu.SemaphoreType.DMA
        return pl.pallas_call(
            functools.partial(kernel, side, chunks_per),
            out_shape=pltpu.VMEM((mats, d, ff), BF16),
            in_specs=[pl.BlockSpec(memory_space=pltpu.HBM)] * 2,
            out_specs=pl.BlockSpec(memory_space=pltpu.VMEM),
            scratch_shapes=[
                pltpu.VMEM((2, tokens, d), BF16),
                pltpu.VMEM((GBUFS, tokens, width), BF16),
                pltpu.VMEM((d, width), F32),
                pltpu.VMEM((OWN_RING, 2, 2, half, LANES), F32),
                pltpu.VMEM((3, 2, chunks, half, LANES), BF16),
                pltpu.VMEM((3, 2, chunks, half, LANES), BF16),
                pltpu.VMEM((PART_RING, 2, GROUP, half, LANES), F32),
                pltpu.VMEM((3, 2, groups, GROUP, quarter, LANES), BF16),
                pltpu.VMEM((3, 2, groups, GROUP, quarter, LANES), BF16),
                dma((2,)),
                dma((GBUFS,)),
                dma((2, HEAD)),
                dma((4,)),
                dma((3, 2, chunks)),
                dma((9, 2, groups)),
            ],
            compiler_params=pltpu.CompilerParams(collective_id=0, has_side_effects=True, vmem_limit_bytes=55_000_000),
            cost_estimate=pl.CostEstimate(flops=2 * mats * tokens * d * ff, bytes_accessed=2 * mats * tokens * (d + ff),
                                          transcendentals=0),
            name="weight_gradients",
        )(a[0], g[0])

    return jax.shard_map(local, mesh=mesh, in_specs=(P(("rep", "dp")), P(("rep", "dp"))), out_specs=P("rep"), check_vma=False)
```

```python
import functools
import math

import jax
import jax.numpy as jnp
from jax import lax
from jax.experimental import pallas as pl
from jax.experimental.pallas import tpu as pltpu
from jax.sharding import PartitionSpec as P

MESH = pl.DeviceIdType.MESH
F32, BF16 = jnp.float32, jnp.bfloat16
LANES = 128
GBUFS = 3
GROUP = 2
HEAD = 4
COMBINE1, OWN1, COMBINE2, OWN2, PASS2 = 4, 8, 10, 14, 18
SEND1, PASS1, DONE1 = 27, 9, 24
OWN_RING = OWN1 // 2 + GROUP
PART_RING = -(-(OWN2 - OWN1) // (2 * GROUP))

def kernel(side, chunks_per, a_ref, g_ref, out, abuf, gbuf, acc, own, send1, recv1, part2, send2, recv2,
           asem, gsem, hsem, ssem, rsem1, rsem2):
    mats, tokens, d = a_ref.shape
    chunks = mats * chunks_per
    groups = chunks // GROUP
    half = d // 2
    quarter = half // side
    width = side * LANES
    cut = -(-half // LANES) * LANES
    strip = g_ref.shape[2] // side
    me = lax.axis_index("dp")
    pos = (me // side, lax.rem(me, side))
    core = lax.rem(lax.axis_index("rep"), 2)

    def device(axis, index):
        return {"dp": index * side + pos[1] if axis == 0 else pos[0] * side + index}

    def wrap(i):
        return lax.rem(i, side)

    def block(i, size):
        return pl.ds(pl.multiple_of(i * size, size), size)

    def parity(c):
        return lax.rem(c + core, 2)

    def step(c):
        return 1 + 2 * parity(c)

    def to(axis, index, src, dst, send_sem, recv_sem):
        return pltpu.make_async_remote_copy(src_ref=src, dst_ref=dst, send_sem=send_sem, recv_sem=recv_sem,
                                            device_id=device(axis, index), device_id_type=MESH)

    def copy_a(n):
        i = lax.rem(n, 2)
        return pltpu.make_async_copy(a_ref.at[n], abuf.at[i], asem.at[i])

    def start_g(t):
        n, j, i = t // chunks_per, lax.rem(t, chunks_per), lax.rem(t, GBUFS)
        for b in range(side):
            cols = pl.ds(pl.multiple_of(b * strip + j * LANES, LANES), LANES)
            pltpu.make_async_copy(g_ref.at[n, :, cols], gbuf.at[i, :, pl.ds(b * LANES, LANES)], gsem.at[i]).start()

    def whole_g(t):
        i = lax.rem(t, GBUFS)
        return pltpu.make_async_copy(g_ref.at[0, :, pl.ds(0, width)], gbuf.at[i], gsem.at[i])

    def head_rows(k):
        return pl.ds(k * (tokens // HEAD), tokens // HEAD)

    def head_a(k):
        return pltpu.make_async_copy(a_ref.at[0, head_rows(k)], abuf.at[0, head_rows(k)], hsem.at[0, k])

    def start_head(k):
        head_a(k).start()
        for b in range(side):
            pltpu.make_async_copy(g_ref.at[0, head_rows(k), pl.ds(b * strip, LANES)],
                                  gbuf.at[0, head_rows(k), pl.ds(b * LANES, LANES)], hsem.at[1, k]).start()

    def wait_head(k):
        head_a(k).wait()
        pltpu.make_async_copy(g_ref.at[0, head_rows(k), pl.ds(0, width)], gbuf.at[0, head_rows(k)], hsem.at[1, k]).wait()

    def product(a, g):
        return lax.dot_general(a, g, (((0,), (0,)), ((), ())), preferred_element_type=F32)

    def hop1(kind, h, c):
        p, s = pos[h], step(c)
        index = wrap(p + s) if kind == 1 else wrap(p + side - s)
        return to(h, index, send1.at[kind, h, c], recv1.at[kind, h, c], ssem.at[0], rsem1.at[kind, h, c])

    def start1(h, t):
        r = lax.rem(t, OWN_RING)
        rows = pl.ds(h * half, half)
        p, s = pos[h], step(t)
        send1[0, h, t] = acc[rows, block(wrap(p + 2), LANES)].astype(BF16)
        send1[1, h, t] = acc[rows, block(wrap(p + s), LANES)].astype(BF16)
        own[r, h, 0] = acc[rows, block(wrap(p + side - s), LANES)]
        own[r, h, 1] = acc[rows, block(p, LANES)]
        hop1(0, h, t).start()
        hop1(1, h, t).start()

    def combine1(c):
        r = lax.rem(c, OWN_RING)
        for h in range(2):
            hop1(0, h, c).wait_recv()
            send1[2, h, c] = (own[r, h, 0] + recv1[0, h, c].astype(F32)).astype(BF16)
            hop1(2, h, c).start()

    def hop2(kind, h, k):
        q, s = pos[1 - h], step(k)
        index = wrap(q + s) if kind == 1 else wrap(q + side - s)
        return to(1 - h, index, send2.at[kind, h, k], recv2.at[kind, h, k], ssem.at[1], rsem2.at[kind, h, k])

    def own1(k):
        r2 = lax.rem(k, PART_RING)
        for h in range(2):
            q, s = pos[1 - h], step(k)
            for i in range(GROUP):
                c = k * GROUP + i
                hop1(1, h, c).wait_recv()
                hop1(2, h, c).wait_recv()
                part2[r2, h, i] = (own[lax.rem(c, OWN_RING), h, 1] + recv1[1, h, c].astype(F32)
                                   + recv1[2, h, c].astype(F32))
                send2[0, h, k, i] = part2[r2, h, i, block(wrap(q + 2), quarter)].astype(BF16)
                send2[1, h, k, i] = part2[r2, h, i, block(wrap(q + s), quarter)].astype(BF16)
            hop2(0, h, k).start()
            hop2(1, h, k).start()

    def combine2(k):
        r2 = lax.rem(k, PART_RING)
        for h in range(2):
            q, s = pos[1 - h], step(k)
            hop2(0, h, k).wait_recv()
            mine = part2[r2, h, :, block(wrap(q + side - s), quarter)]
            send2[2, h, k] = (mine + recv2[0, h, k].astype(F32)).astype(BF16)
            hop2(2, h, k).start()

    def columns(b, c, count):
        first = b * strip + lax.rem(c, chunks_per) * LANES
        return pl.ds(pl.multiple_of(first, count * LANES), count * LANES)

    def gather2(kind, h, k):
        q, s, c = pos[1 - h], step(k), k * GROUP
        owner = wrap(q + side - s) if kind == 2 else q
        index = wrap(q + (1, side - 1, s)[kind])
        rows = pl.ds(pl.multiple_of(h * half + owner * quarter, 16), quarter)
        ref = out.at[c // chunks_per, rows, columns(pos[h], c, GROUP)]
        return to(1 - h, index, ref, ref, ssem.at[2], rsem2.at[3 + kind, h, k])

    def wait2(kind, h, k):
        c = k * GROUP
        ref = out.at[c // chunks_per, pl.ds(h * half, quarter), columns(pos[h], c, GROUP)]
        to(h, pos[h], ref, ref, ssem.at[2], rsem2.at[3 + kind, h, k]).wait_recv()

    def own2(k):
        r2 = lax.rem(k, PART_RING)
        for h in range(2):
            q = pos[1 - h]
            hop2(1, h, k).wait_recv()
            hop2(2, h, k).wait_recv()
            rows = pl.ds(pl.multiple_of(h * half + q * quarter, 16), quarter)
            for i in range(GROUP):
                c = k * GROUP + i
                total = (part2[r2, h, i, block(q, quarter)] + recv2[1, h, k, i].astype(F32)
                         + recv2[2, h, k, i].astype(F32))
                out[c // chunks_per, rows, columns(pos[h], c, 1)] = total.astype(BF16)
            gather2(0, h, k).start()
            gather2(1, h, k).start()

    def pass2(k):
        for h in range(2):
            wait2(parity(k), h, k)
            gather2(2, h, k).start()

    def gather1(kind, h, k):
        p, s, c = pos[h], step(k), k * GROUP
        owner = wrap(p + side - s) if kind == 2 else p
        index = wrap(p + (1, side - 1, s)[kind])
        ref = out.at[c // chunks_per, pl.ds(h * half, half), columns(owner, c, GROUP)]
        return to(h, index, ref, ref, ssem.at[3], rsem2.at[6 + kind, h, k])

    def wait1(kind, h, k):
        c = k * GROUP
        ref = out.at[c // chunks_per, pl.ds(h * half, half), columns(pos[h], c, GROUP)]
        to(h, pos[h], ref, ref, ssem.at[3], rsem2.at[6 + kind, h, k]).wait_recv()

    def send_whole(k):
        for h in range(2):
            wait2(1 - parity(k), h, k)
            wait2(2, h, k)
            gather1(0, h, k).start()
            gather1(1, h, k).start()

    def pass1(k):
        for h in range(2):
            wait1(parity(k), h, k)
            gather1(2, h, k).start()

    def done1(k):
        for h in range(2):
            wait1(1 - parity(k), h, k)
            wait1(2, h, k)

    def at(do, t, now, first, every, count):
        if (now - first) % 2:
            return
        late = 2 * t + now - first

        @pl.when((late >= 0) & (late < every * count) & (lax.rem(late, every) == 0))
        def _():
            do(late // every)

    def steps(t, now):
        span, last = 2 * GROUP, 2 * GROUP - 1
        at(done1, t, now, SEND1 + DONE1, span, groups)
        at(pass1, t, now, SEND1 + PASS1, span, groups)
        at(send_whole, t, now, SEND1, span, groups)
        at(pass2, t, now, last + PASS2, span, groups)
        at(own2, t, now, last + OWN2, span, groups)
        at(combine2, t, now, last + COMBINE2, span, groups)
        at(own1, t, now, last + OWN1, span, groups)
        at(combine1, t, now, 1 + COMBINE1, 2, chunks)

    barrier = pltpu.get_barrier_semaphore()
    neighbours = [device(axis, wrap(pos[axis] + k)) for axis in range(2) for k in (1, side - 1)]
    for nb in neighbours:
        pl.semaphore_signal(barrier, inc=1, device_id=nb, device_id_type=MESH)
    for k in range(HEAD):
        start_head(k)
    upper = pl.ds(0, cut)
    lower = pl.ds(cut, d - cut)
    for k in range(HEAD):
        wait_head(k)
        if k == 0:
            start_g(1)
        part = product(abuf[0, head_rows(k), upper], gbuf[0, head_rows(k)])
        acc[upper] = part if k == 0 else acc[upper] + part
    pl.semaphore_wait(barrier, len(neighbours))
    start1(0, 0)
    acc[lower] = product(abuf[0, :, lower], gbuf[0])
    start1(1, 0)
    start_g(2)
    copy_a(1).start()

    def compute_slot(t, carry):
        steps(t, 0)

        @pl.when(t + GBUFS - 1 < chunks)
        def _():
            start_g(t + GBUFS - 1)

        @pl.when(lax.rem(t, chunks_per) == 0)
        def _():
            n = t // chunks_per

            @pl.when(n + 1 < mats)
            def _():
                copy_a(n + 1).start()

            copy_a(n).wait()

        whole_g(t).wait()
        i, j = lax.rem(t // chunks_per, 2), lax.rem(t, GBUFS)
        acc[upper] = product(abuf[i, :, upper], gbuf[j])
        steps(t, 1)
        acc[lower] = product(abuf[i, :, lower], gbuf[j])
        start1(0, t)
        start1(1, t)
        return carry

    lax.fori_loop(1, chunks, compute_slot, 0)

    def gather_slot(t, carry):
        steps(t, 0)
        steps(t, 1)
        return carry

    end = SEND1 + DONE1 + 2 * (chunks - GROUP)
    lax.fori_loop(chunks, end // 2 + 1, gather_slot, 0)

    to(0, pos[0], send1, recv1, ssem.at[0], rsem1.at[0, 0, 0]).wait_send()
    to(0, pos[0], send2, recv2, ssem.at[1], rsem2.at[0, 0, 0]).wait_send()
    to(0, pos[0], send2, recv2, ssem.at[2], rsem2.at[0, 0, 0]).wait_send()
    to(0, pos[0], send1, recv1, ssem.at[3], rsem2.at[0, 0, 0]).wait_send()


def solution(mesh):
    side = math.isqrt(mesh.shape["dp"])

    def local(a, g):
        _, mats, tokens, d = a.shape
        ff = g.shape[3]
        width = side * LANES
        chunks_per = ff // width
        chunks = mats * chunks_per
        groups = chunks // GROUP
        half = d // 2
        quarter = half // side
        dma = pltpu.SemaphoreType.DMA
        return pl.pallas_call(
            functools.partial(kernel, side, chunks_per),
            out_shape=pltpu.VMEM((mats, d, ff), BF16),
            in_specs=[pl.BlockSpec(memory_space=pltpu.HBM)] * 2,
            out_specs=pl.BlockSpec(memory_space=pltpu.VMEM),
            scratch_shapes=[
                pltpu.VMEM((2, tokens, d), BF16),
                pltpu.VMEM((GBUFS, tokens, width), BF16),
                pltpu.VMEM((d, width), F32),
                pltpu.VMEM((OWN_RING, 2, 2, half, LANES), F32),
                pltpu.VMEM((3, 2, chunks, half, LANES), BF16),
                pltpu.VMEM((3, 2, chunks, half, LANES), BF16),
                pltpu.VMEM((PART_RING, 2, GROUP, half, LANES), F32),
                pltpu.VMEM((3, 2, groups, GROUP, quarter, LANES), BF16),
                pltpu.VMEM((3, 2, groups, GROUP, quarter, LANES), BF16),
                dma((2,)),
                dma((GBUFS,)),
                dma((2, HEAD)),
                dma((4,)),
                dma((3, 2, chunks)),
                dma((9, 2, groups)),
            ],
            compiler_params=pltpu.CompilerParams(collective_id=0, has_side_effects=True, vmem_limit_bytes=55_000_000),
            cost_estimate=pl.CostEstimate(flops=2 * mats * tokens * d * ff, bytes_accessed=2 * mats * tokens * (d + ff),
                                          transcendentals=0),
            name="weight_gradients",
        )(a[0], g[0])

    return jax.shard_map(local, mesh=mesh, in_specs=(P(("rep", "dp")), P(("rep", "dp"))), out_specs=P("rep"), check_vma=False)
```

```python
import functools
import math

import jax
import jax.numpy as jnp
from jax import lax
from jax.experimental import pallas as pl
from jax.experimental.pallas import tpu as pltpu
from jax.sharding import PartitionSpec as P

MESH = pl.DeviceIdType.MESH
F32, BF16 = jnp.float32, jnp.bfloat16
LANES = 128
GBUFS = 3
GROUP = 2
HEAD = 4
COMBINE1, OWN1, COMBINE2, OWN2, PASS2 = 4, 8, 11, 15, 19
SEND1, PASS1, DONE1 = 27, 9, 24
ACC_RING = OWN1 // 2 + GROUP
PART_RING = -(-(OWN2 - OWN1) // (2 * GROUP))

def kernel(side, chunks_per, a_ref, g_ref, out, abuf, gbuf, acc, send1, recv1, part2, send2, recv2,
           asem, gsem, hsem, ssem, rsem1, rsem2):
    mats, tokens, d = a_ref.shape
    chunks = mats * chunks_per
    groups = chunks // GROUP
    half = d // 2
    quarter = half // side
    width = side * LANES
    cut = -(-half // LANES) * LANES
    strip = g_ref.shape[2] // side
    me = lax.axis_index("dp")
    pos = (me // side, lax.rem(me, side))
    core = lax.rem(lax.axis_index("rep"), 2)

    def device(axis, index):
        return {"dp": index * side + pos[1] if axis == 0 else pos[0] * side + index}

    def wrap(i):
        return lax.rem(i, side)

    def block(i, size):
        return pl.ds(pl.multiple_of(i * size, size), size)

    def parity(c):
        return lax.rem(c + core, 2)

    def step(c):
        return 1 + 2 * parity(c)

    def to(axis, index, src, dst, send_sem, recv_sem):
        return pltpu.make_async_remote_copy(src_ref=src, dst_ref=dst, send_sem=send_sem, recv_sem=recv_sem,
                                            device_id=device(axis, index), device_id_type=MESH)

    def copy_a(n):
        i = lax.rem(n, 2)
        return pltpu.make_async_copy(a_ref.at[n], abuf.at[i], asem.at[i])

    def start_g(t):
        n, j, i = t // chunks_per, lax.rem(t, chunks_per), lax.rem(t, GBUFS)
        for b in range(side):
            cols = pl.ds(pl.multiple_of(b * strip + j * LANES, LANES), LANES)
            pltpu.make_async_copy(g_ref.at[n, :, cols], gbuf.at[i, :, pl.ds(b * LANES, LANES)], gsem.at[i]).start()

    def whole_g(t):
        i = lax.rem(t, GBUFS)
        return pltpu.make_async_copy(g_ref.at[0, :, pl.ds(0, width)], gbuf.at[i], gsem.at[i])

    def head_rows(k):
        return pl.ds(k * (tokens // HEAD), tokens // HEAD)

    def head_a(k):
        part = (0, head_rows(k), pl.ds(0, cut))
        return pltpu.make_async_copy(a_ref.at[part], abuf.at[part], hsem.at[0, k])

    def rest_a():
        part = (0, slice(None), pl.ds(cut, d - cut))
        return pltpu.make_async_copy(a_ref.at[part], abuf.at[part], asem.at[0])

    def start_head(k):
        head_a(k).start()
        for b in range(side):
            pltpu.make_async_copy(g_ref.at[0, head_rows(k), pl.ds(b * strip, LANES)],
                                  gbuf.at[0, head_rows(k), pl.ds(b * LANES, LANES)], hsem.at[1, k]).start()

    def wait_head(k):
        head_a(k).wait()
        pltpu.make_async_copy(g_ref.at[0, head_rows(k), pl.ds(0, width)], gbuf.at[0, head_rows(k)], hsem.at[1, k]).wait()

    def product(a, g):
        return lax.dot_general(a, g, (((0,), (0,)), ((), ())), preferred_element_type=F32)

    def hop1(kind, h, c):
        p, s = pos[h], step(c)
        index = wrap(p + s) if kind == 1 else wrap(p + side - s)
        return to(h, index, send1.at[kind, h, c], recv1.at[kind, h, c], ssem.at[0], rsem1.at[kind, h, c])

    def term(h, b, t):
        return acc[lax.rem(t, ACC_RING), pl.ds(h * half, half), block(b, LANES)]

    def start1(h, t):
        p, s = pos[h], step(t)
        send1[0, h, t] = term(h, wrap(p + 2), t).astype(BF16)
        send1[1, h, t] = term(h, wrap(p + s), t).astype(BF16)
        hop1(0, h, t).start()
        hop1(1, h, t).start()

    def combine1(c):
        for h in range(2):
            p, s = pos[h], step(c)
            hop1(0, h, c).wait_recv()
            send1[2, h, c] = (term(h, wrap(p + side - s), c) + recv1[0, h, c].astype(F32)).astype(BF16)
            hop1(2, h, c).start()

    def hop2(kind, h, k):
        q, s = pos[1 - h], step(k)
        index = wrap(q + s) if kind == 1 else wrap(q + side - s)
        return to(1 - h, index, send2.at[kind, h, k], recv2.at[kind, h, k], ssem.at[1], rsem2.at[kind, h, k])

    def own1(k):
        r2 = lax.rem(k, PART_RING)
        for h in range(2):
            q, s = pos[1 - h], step(k)
            for i in range(GROUP):
                c = k * GROUP + i
                hop1(1, h, c).wait_recv()
                hop1(2, h, c).wait_recv()
                part2[r2, h, i] = term(h, pos[h], c) + recv1[1, h, c].astype(F32) + recv1[2, h, c].astype(F32)
                send2[0, h, k, i] = part2[r2, h, i, block(wrap(q + 2), quarter)].astype(BF16)
                send2[1, h, k, i] = part2[r2, h, i, block(wrap(q + s), quarter)].astype(BF16)
            hop2(0, h, k).start()
            hop2(1, h, k).start()

    def combine2(k):
        r2 = lax.rem(k, PART_RING)
        for h in range(2):
            q, s = pos[1 - h], step(k)
            hop2(0, h, k).wait_recv()
            mine = part2[r2, h, :, block(wrap(q + side - s), quarter)]
            send2[2, h, k] = (mine + recv2[0, h, k].astype(F32)).astype(BF16)
            hop2(2, h, k).start()

    def columns(b, c, count):
        first = b * strip + lax.rem(c, chunks_per) * LANES
        return pl.ds(pl.multiple_of(first, count * LANES), count * LANES)

    def gather2(kind, h, k):
        q, s, c = pos[1 - h], step(k), k * GROUP
        owner = wrap(q + side - s) if kind == 2 else q
        index = wrap(q + (1, side - 1, s)[kind])
        rows = pl.ds(pl.multiple_of(h * half + owner * quarter, 16), quarter)
        ref = out.at[c // chunks_per, rows, columns(pos[h], c, GROUP)]
        return to(1 - h, index, ref, ref, ssem.at[2], rsem2.at[3 + kind, h, k])

    def wait2(kind, h, k):
        c = k * GROUP
        ref = out.at[c // chunks_per, pl.ds(h * half, quarter), columns(pos[h], c, GROUP)]
        to(h, pos[h], ref, ref, ssem.at[2], rsem2.at[3 + kind, h, k]).wait_recv()

    def own2(k):
        r2 = lax.rem(k, PART_RING)
        for h in range(2):
            q = pos[1 - h]
            hop2(1, h, k).wait_recv()
            hop2(2, h, k).wait_recv()
            rows = pl.ds(pl.multiple_of(h * half + q * quarter, 16), quarter)
            for i in range(GROUP):
                c = k * GROUP + i
                total = (part2[r2, h, i, block(q, quarter)] + recv2[1, h, k, i].astype(F32)
                         + recv2[2, h, k, i].astype(F32))
                out[c // chunks_per, rows, columns(pos[h], c, 1)] = total.astype(BF16)
            gather2(0, h, k).start()
            gather2(1, h, k).start()

    def pass2(k):
        for h in range(2):
            wait2(parity(k), h, k)
            gather2(2, h, k).start()

    def gather1(kind, h, k):
        p, s, c = pos[h], step(k), k * GROUP
        owner = wrap(p + side - s) if kind == 2 else p
        index = wrap(p + (1, side - 1, s)[kind])
        ref = out.at[c // chunks_per, pl.ds(h * half, half), columns(owner, c, GROUP)]
        return to(h, index, ref, ref, ssem.at[3], rsem2.at[6 + kind, h, k])

    def wait1(kind, h, k):
        c = k * GROUP
        ref = out.at[c // chunks_per, pl.ds(h * half, half), columns(pos[h], c, GROUP)]
        to(h, pos[h], ref, ref, ssem.at[3], rsem2.at[6 + kind, h, k]).wait_recv()

    def send_whole(k):
        for h in range(2):
            wait2(1 - parity(k), h, k)
            wait2(2, h, k)
            gather1(0, h, k).start()
            gather1(1, h, k).start()

    def pass1(k):
        for h in range(2):
            wait1(parity(k), h, k)
            gather1(2, h, k).start()

    def done1(k):
        for h in range(2):
            wait1(1 - parity(k), h, k)
            wait1(2, h, k)

    def at(do, t, now, first, every, count):
        if (now - first) % 2:
            return
        late = 2 * t + now - first

        @pl.when((late >= 0) & (late < every * count) & (lax.rem(late, every) == 0))
        def _():
            do(late // every)

    def steps(t, now):
        span, last = 2 * GROUP, 2 * GROUP - 1
        at(pass1, t, now, SEND1 + PASS1, span, groups)
        at(pass2, t, now, last + PASS2, span, groups)
        at(own2, t, now, last + OWN2, span, groups)
        at(combine2, t, now, last + COMBINE2, span, groups)
        at(own1, t, now, last + OWN1, span, groups)
        at(combine1, t, now, 1 + COMBINE1, 2, chunks)
        at(send_whole, t, now, SEND1, span, groups)
        at(done1, t, now, SEND1 + DONE1, span, groups)

    barrier = pltpu.get_barrier_semaphore()
    neighbours = [device(axis, wrap(pos[axis] + k)) for axis in range(2) for k in (1, side - 1)]
    for nb in neighbours:
        pl.semaphore_signal(barrier, inc=1, device_id=nb, device_id_type=MESH)
    for k in range(HEAD):
        start_head(k)
    rest_a().start()
    upper = pl.ds(0, cut)
    lower = pl.ds(cut, d - cut)
    for k in range(HEAD):
        wait_head(k)
        if k == 0:
            start_g(1)
        part = product(abuf[0, head_rows(k), upper], gbuf[0, head_rows(k)])
        acc[0, upper] = part if k == 0 else acc[0, upper] + part
    pl.semaphore_wait(barrier, len(neighbours))
    start1(0, 0)
    rest_a().wait()
    acc[0, lower] = product(abuf[0, :, lower], gbuf[0])
    start1(1, 0)
    start_g(2)
    copy_a(1).start()

    def compute_slot(t, carry):
        steps(t, 0)

        @pl.when(t + GBUFS - 1 < chunks)
        def _():
            start_g(t + GBUFS - 1)

        @pl.when(lax.rem(t, chunks_per) == 0)
        def _():
            n = t // chunks_per

            @pl.when(n + 1 < mats)
            def _():
                copy_a(n + 1).start()

            copy_a(n).wait()

        whole_g(t).wait()
        i, j, r = lax.rem(t // chunks_per, 2), lax.rem(t, GBUFS), lax.rem(t, ACC_RING)
        acc[r, upper] = product(abuf[i, :, upper], gbuf[j])
        steps(t, 1)
        acc[r, lower] = product(abuf[i, :, lower], gbuf[j])
        start1(0, t)
        start1(1, t)
        return carry

    lax.fori_loop(1, chunks, compute_slot, 0)

    def gather_slot(t, carry):
        steps(t, 0)
        steps(t, 1)
        return carry

    end = SEND1 + DONE1 + 2 * (chunks - GROUP)
    lax.fori_loop(chunks, end // 2 + 1, gather_slot, 0)

    to(0, pos[0], send1, recv1, ssem.at[0], rsem1.at[0, 0, 0]).wait_send()
    to(0, pos[0], send2, recv2, ssem.at[1], rsem2.at[0, 0, 0]).wait_send()
    to(0, pos[0], send2, recv2, ssem.at[2], rsem2.at[0, 0, 0]).wait_send()
    to(0, pos[0], send1, recv1, ssem.at[3], rsem2.at[0, 0, 0]).wait_send()


def solution(mesh):
    side = math.isqrt(mesh.shape["dp"])

    def local(a, g):
        _, mats, tokens, d = a.shape
        ff = g.shape[3]
        width = side * LANES
        chunks_per = ff // width
        chunks = mats * chunks_per
        groups = chunks // GROUP
        half = d // 2
        quarter = half // side
        dma = pltpu.SemaphoreType.DMA
        return pl.pallas_call(
            functools.partial(kernel, side, chunks_per),
            out_shape=pltpu.VMEM((mats, d, ff), BF16),
            in_specs=[pl.BlockSpec(memory_space=pltpu.HBM)] * 2,
            out_specs=pl.BlockSpec(memory_space=pltpu.VMEM),
            scratch_shapes=[
                pltpu.VMEM((2, tokens, d), BF16),
                pltpu.VMEM((GBUFS, tokens, width), BF16),
                pltpu.VMEM((ACC_RING, d, width), F32),
                pltpu.VMEM((3, 2, chunks, half, LANES), BF16),
                pltpu.VMEM((3, 2, chunks, half, LANES), BF16),
                pltpu.VMEM((PART_RING, 2, GROUP, half, LANES), F32),
                pltpu.VMEM((3, 2, groups, GROUP, quarter, LANES), BF16),
                pltpu.VMEM((3, 2, groups, GROUP, quarter, LANES), BF16),
                dma((2,)),
                dma((GBUFS,)),
                dma((2, HEAD)),
                dma((4,)),
                dma((3, 2, chunks)),
                dma((9, 2, groups)),
            ],
            compiler_params=pltpu.CompilerParams(collective_id=0, has_side_effects=True, vmem_limit_bytes=55_000_000),
            cost_estimate=pl.CostEstimate(flops=2 * mats * tokens * d * ff, bytes_accessed=2 * mats * tokens * (d + ff),
                                          transcendentals=0),
            name="weight_gradients",
        )(a[0], g[0])

    return jax.shard_map(local, mesh=mesh, in_specs=(P(("rep", "dp")), P(("rep", "dp"))), out_specs=P("rep"), check_vma=False)
```

```python
import functools
import math

import jax
import jax.numpy as jnp
from jax import lax
from jax.experimental import pallas as pl
from jax.experimental.pallas import tpu as pltpu
from jax.sharding import PartitionSpec as P

MESH = pl.DeviceIdType.MESH
F32, BF16 = jnp.float32, jnp.bfloat16
LANES = 128
GBUFS = 3
GROUP = 2
HEAD = 4
COMBINE1, OWN1, COMBINE2, OWN2, PASS2 = 4, 8, 11, 14, 18
SEND1, PASS1, DONE1 = 28, 9, 24
ACC_RING = OWN1 // 2 + GROUP
PART_RING = -(-(OWN2 - OWN1) // (2 * GROUP))

def kernel(side, chunks_per, a_ref, g_ref, out, abuf, gbuf, acc, send1, recv1, part2, send2, recv2,
           asem, gsem, hsem, ssem, rsem1, rsem2):
    mats, tokens, d = a_ref.shape
    chunks = mats * chunks_per
    groups = chunks // GROUP
    half = d // 2
    quarter = half // side
    width = side * LANES
    cut = -(-half // LANES) * LANES
    strip = g_ref.shape[2] // side
    me = lax.axis_index("dp")
    pos = (me // side, lax.rem(me, side))
    core = lax.rem(lax.axis_index("rep"), 2)

    def device(axis, index):
        return {"dp": index * side + pos[1] if axis == 0 else pos[0] * side + index}

    def wrap(i):
        return lax.rem(i, side)

    def block(i, size):
        return pl.ds(pl.multiple_of(i * size, size), size)

    def parity(c):
        return lax.rem(c + core, 2)

    def step(c):
        return 1 + 2 * parity(c)

    def to(axis, index, src, dst, send_sem, recv_sem):
        return pltpu.make_async_remote_copy(src_ref=src, dst_ref=dst, send_sem=send_sem, recv_sem=recv_sem,
                                            device_id=device(axis, index), device_id_type=MESH)

    def copy_a(n):
        i = lax.rem(n, 2)
        return pltpu.make_async_copy(a_ref.at[n], abuf.at[i], asem.at[i])

    def start_g(t):
        n, j, i = t // chunks_per, lax.rem(t, chunks_per), lax.rem(t, GBUFS)
        for b in range(side):
            cols = pl.ds(pl.multiple_of(b * strip + j * LANES, LANES), LANES)
            pltpu.make_async_copy(g_ref.at[n, :, cols], gbuf.at[i, :, pl.ds(b * LANES, LANES)], gsem.at[i]).start()

    def whole_g(t):
        i = lax.rem(t, GBUFS)
        return pltpu.make_async_copy(g_ref.at[0, :, pl.ds(0, width)], gbuf.at[i], gsem.at[i])

    def head_rows(k):
        return pl.ds(k * (tokens // HEAD), tokens // HEAD)

    def head_a(k):
        part = (0, head_rows(k), pl.ds(0, cut))
        return pltpu.make_async_copy(a_ref.at[part], abuf.at[part], hsem.at[0, k])

    def rest_a():
        part = (0, slice(None), pl.ds(cut, d - cut))
        return pltpu.make_async_copy(a_ref.at[part], abuf.at[part], asem.at[0])

    def start_head(k):
        head_a(k).start()
        for b in range(side):
            pltpu.make_async_copy(g_ref.at[0, head_rows(k), pl.ds(b * strip, LANES)],
                                  gbuf.at[0, head_rows(k), pl.ds(b * LANES, LANES)], hsem.at[1, k]).start()

    def wait_head(k):
        head_a(k).wait()
        pltpu.make_async_copy(g_ref.at[0, head_rows(k), pl.ds(0, width)], gbuf.at[0, head_rows(k)], hsem.at[1, k]).wait()

    def product(a, g):
        return lax.dot_general(a, g, (((0,), (0,)), ((), ())), preferred_element_type=F32)

    def hop1(kind, h, c):
        p, s = pos[h], step(c)
        index = wrap(p + s) if kind == 1 else wrap(p + side - s)
        return to(h, index, send1.at[kind, h, c], recv1.at[kind, h, c], ssem.at[0], rsem1.at[kind, h, c])

    def term(h, b, t):
        return acc[lax.rem(t, ACC_RING), pl.ds(h * half, half), block(b, LANES)]

    def start1(h, t):
        p, s = pos[h], step(t)
        send1[0, h, t] = term(h, wrap(p + 2), t).astype(BF16)
        send1[1, h, t] = term(h, wrap(p + s), t).astype(BF16)
        hop1(0, h, t).start()
        hop1(1, h, t).start()

    def combine1(c):
        for h in range(2):
            p, s = pos[h], step(c)
            hop1(0, h, c).wait_recv()
            send1[2, h, c] = (term(h, wrap(p + side - s), c) + recv1[0, h, c].astype(F32)).astype(BF16)
            hop1(2, h, c).start()

    def hop2(kind, h, k):
        q, s = pos[1 - h], step(k)
        index = wrap(q + s) if kind == 1 else wrap(q + side - s)
        return to(1 - h, index, send2.at[kind, h, k], recv2.at[kind, h, k], ssem.at[1], rsem2.at[kind, h, k])

    def own1(k):
        r2 = lax.rem(k, PART_RING)
        for h in range(2):
            q, s = pos[1 - h], step(k)
            for i in range(GROUP):
                c = k * GROUP + i
                hop1(1, h, c).wait_recv()
                hop1(2, h, c).wait_recv()
                part2[r2, h, i] = term(h, pos[h], c) + recv1[1, h, c].astype(F32) + recv1[2, h, c].astype(F32)
                send2[0, h, k, i] = part2[r2, h, i, block(wrap(q + 2), quarter)].astype(BF16)
                send2[1, h, k, i] = part2[r2, h, i, block(wrap(q + s), quarter)].astype(BF16)
            hop2(0, h, k).start()
            hop2(1, h, k).start()

    def combine2(k):
        r2 = lax.rem(k, PART_RING)
        for h in range(2):
            q, s = pos[1 - h], step(k)
            hop2(0, h, k).wait_recv()
            mine = part2[r2, h, :, block(wrap(q + side - s), quarter)]
            send2[2, h, k] = (mine + recv2[0, h, k].astype(F32)).astype(BF16)
            hop2(2, h, k).start()

    def columns(b, c, count):
        first = b * strip + lax.rem(c, chunks_per) * LANES
        return pl.ds(pl.multiple_of(first, count * LANES), count * LANES)

    def gather2(kind, h, k):
        q, s, c = pos[1 - h], step(k), k * GROUP
        owner = wrap(q + side - s) if kind == 2 else q
        index = wrap(q + (1, side - 1, s)[kind])
        rows = pl.ds(pl.multiple_of(h * half + owner * quarter, 16), quarter)
        ref = out.at[c // chunks_per, rows, columns(pos[h], c, GROUP)]
        return to(1 - h, index, ref, ref, ssem.at[2], rsem2.at[3 + kind, h, k])

    def wait2(kind, h, k):
        c = k * GROUP
        ref = out.at[c // chunks_per, pl.ds(h * half, quarter), columns(pos[h], c, GROUP)]
        to(h, pos[h], ref, ref, ssem.at[2], rsem2.at[3 + kind, h, k]).wait_recv()

    def own2(k):
        r2 = lax.rem(k, PART_RING)
        for h in range(2):
            q = pos[1 - h]
            hop2(1, h, k).wait_recv()
            hop2(2, h, k).wait_recv()
            rows = pl.ds(pl.multiple_of(h * half + q * quarter, 16), quarter)
            for i in range(GROUP):
                c = k * GROUP + i
                total = (part2[r2, h, i, block(q, quarter)] + recv2[1, h, k, i].astype(F32)
                         + recv2[2, h, k, i].astype(F32))
                out[c // chunks_per, rows, columns(pos[h], c, 1)] = total.astype(BF16)
            gather2(0, h, k).start()
            gather2(1, h, k).start()

    def pass2(k):
        for h in range(2):
            wait2(parity(k), h, k)
            gather2(2, h, k).start()

    def gather1(kind, h, k):
        p, s, c = pos[h], step(k), k * GROUP
        owner = wrap(p + side - s) if kind == 2 else p
        index = wrap(p + (1, side - 1, s)[kind])
        ref = out.at[c // chunks_per, pl.ds(h * half, half), columns(owner, c, GROUP)]
        return to(h, index, ref, ref, ssem.at[3], rsem2.at[6 + kind, h, k])

    def wait1(kind, h, k):
        c = k * GROUP
        ref = out.at[c // chunks_per, pl.ds(h * half, half), columns(pos[h], c, GROUP)]
        to(h, pos[h], ref, ref, ssem.at[3], rsem2.at[6 + kind, h, k]).wait_recv()

    def send_whole(k):
        for h in range(2):
            wait2(1 - parity(k), h, k)
            wait2(2, h, k)
            gather1(0, h, k).start()
            gather1(1, h, k).start()

    def pass1(k):
        for h in range(2):
            wait1(parity(k), h, k)
            gather1(2, h, k).start()

    def done1(k):
        for h in range(2):
            wait1(1 - parity(k), h, k)
            wait1(2, h, k)

    def at(do, t, now, first, every, count):
        if (now - first) % 2:
            return
        late = 2 * t + now - first

        @pl.when((late >= 0) & (late < every * count) & (lax.rem(late, every) == 0))
        def _():
            do(late // every)

    def steps(t, now):
        span, last = 2 * GROUP, 2 * GROUP - 1
        at(pass1, t, now, SEND1 + PASS1, span, groups)
        at(pass2, t, now, last + PASS2, span, groups)
        at(own2, t, now, last + OWN2, span, groups)
        at(combine2, t, now, last + COMBINE2, span, groups)
        at(own1, t, now, last + OWN1, span, groups)
        at(combine1, t, now, 1 + COMBINE1, 2, chunks)
        at(send_whole, t, now, SEND1, span, groups)
        at(done1, t, now, SEND1 + DONE1, span, groups)

    barrier = pltpu.get_barrier_semaphore()
    neighbours = [device(axis, wrap(pos[axis] + k)) for axis in range(2) for k in (1, side - 1)]
    for nb in neighbours:
        pl.semaphore_signal(barrier, inc=1, device_id=nb, device_id_type=MESH)
    for k in range(HEAD):
        start_head(k)
    rest_a().start()
    upper = pl.ds(0, cut)
    lower = pl.ds(cut, d - cut)
    for k in range(HEAD):
        wait_head(k)
        if k == 0:
            start_g(1)
        part = product(abuf[0, head_rows(k), upper], gbuf[0, head_rows(k)])
        acc[0, upper] = part if k == 0 else acc[0, upper] + part
    pl.semaphore_wait(barrier, len(neighbours))
    start1(0, 0)
    rest_a().wait()
    acc[0, lower] = product(abuf[0, :, lower], gbuf[0])
    start1(1, 0)
    start_g(2)
    copy_a(1).start()

    def compute_slot(t, carry):
        steps(t, 0)

        @pl.when(t + GBUFS - 1 < chunks)
        def _():
            start_g(t + GBUFS - 1)

        @pl.when(lax.rem(t, chunks_per) == 0)
        def _():
            n = t // chunks_per

            @pl.when(n + 1 < mats)
            def _():
                copy_a(n + 1).start()

            copy_a(n).wait()

        whole_g(t).wait()
        i, j, r = lax.rem(t // chunks_per, 2), lax.rem(t, GBUFS), lax.rem(t, ACC_RING)
        acc[r, upper] = product(abuf[i, :, upper], gbuf[j])
        steps(t, 1)
        start1(0, t)
        acc[r, lower] = product(abuf[i, :, lower], gbuf[j])
        start1(1, t)
        return carry

    lax.fori_loop(1, chunks, compute_slot, 0)

    def gather_slot(t, carry):
        steps(t, 0)
        steps(t, 1)
        return carry

    end = SEND1 + DONE1 + 2 * (chunks - GROUP)
    lax.fori_loop(chunks, end // 2 + 1, gather_slot, 0)

    to(0, pos[0], send1, recv1, ssem.at[0], rsem1.at[0, 0, 0]).wait_send()
    to(0, pos[0], send2, recv2, ssem.at[1], rsem2.at[0, 0, 0]).wait_send()
    to(0, pos[0], send2, recv2, ssem.at[2], rsem2.at[0, 0, 0]).wait_send()
    to(0, pos[0], send1, recv1, ssem.at[3], rsem2.at[0, 0, 0]).wait_send()


def solution(mesh):
    side = math.isqrt(mesh.shape["dp"])

    def local(a, g):
        _, mats, tokens, d = a.shape
        ff = g.shape[3]
        width = side * LANES
        chunks_per = ff // width
        chunks = mats * chunks_per
        groups = chunks // GROUP
        half = d // 2
        quarter = half // side
        dma = pltpu.SemaphoreType.DMA
        return pl.pallas_call(
            functools.partial(kernel, side, chunks_per),
            out_shape=pltpu.VMEM((mats, d, ff), BF16),
            in_specs=[pl.BlockSpec(memory_space=pltpu.HBM)] * 2,
            out_specs=pl.BlockSpec(memory_space=pltpu.VMEM),
            scratch_shapes=[
                pltpu.VMEM((2, tokens, d), BF16),
                pltpu.VMEM((GBUFS, tokens, width), BF16),
                pltpu.VMEM((ACC_RING, d, width), F32),
                pltpu.VMEM((3, 2, chunks, half, LANES), BF16),
                pltpu.VMEM((3, 2, chunks, half, LANES), BF16),
                pltpu.VMEM((PART_RING, 2, GROUP, half, LANES), F32),
                pltpu.VMEM((3, 2, groups, GROUP, quarter, LANES), BF16),
                pltpu.VMEM((3, 2, groups, GROUP, quarter, LANES), BF16),
                dma((2,)),
                dma((GBUFS,)),
                dma((2, HEAD)),
                dma((4,)),
                dma((3, 2, chunks)),
                dma((9, 2, groups)),
            ],
            compiler_params=pltpu.CompilerParams(collective_id=0, has_side_effects=True, vmem_limit_bytes=55_000_000),
            cost_estimate=pl.CostEstimate(flops=2 * mats * tokens * d * ff, bytes_accessed=2 * mats * tokens * (d + ff),
                                          transcendentals=0),
            name="weight_gradients",
        )(a[0], g[0])

    return jax.shard_map(local, mesh=mesh, in_specs=(P(("rep", "dp")), P(("rep", "dp"))), out_specs=P("rep"), check_vma=False)
```
